32 devices in a mesh: edp: 2 (over x), ep: 16 (over z, y, core).
Axes of the slice: x: 2, y: 2, z: 4, core: 2. Of those that a mesh axis runs over, the one named last changes fastest.
Arguments:
- attn_input: bfloat16 [4096, 3584], P(('edp', 'ep')), may hold values from -6 to 6
- kv_gain: float32 [3584], replicated, may hold values from 0.25 to 1.75
- latent_cot: bfloat16 [4096, 512], P(('edp', 'ep')), may hold values from -0.09375 to 0.09375
- attn_resid: float32 [3584, 512], P(('edp', 'ep')), may hold values from -4 to 4
- moe_input: bfloat16 [4096, 3584], P(('edp', 'ep')), may hold values from -6 to 6
- moe_cot: bfloat16 [4096, 3584], P(('edp', 'ep')), may hold values from -0.125 to 0.125
- expert_ids: int32 [4096, 2], P(('edp', 'ep')), may hold values from 0 to 3, all different within a row; in each aligned block of 128 rows (0 to 127, 128 to 255, ...) at most 80 rows name the same one
- gate_probs: float32 [4096, 2], P(('edp', 'ep')), may hold values from 0.2 to 1
- w_gate: bfloat16 [3584, 4096], P(None, 'ep'), may hold values from -0.09375 to 0.09375
- w_up: bfloat16 [3584, 4096], P(None, 'ep'), may hold values from -0.09375 to 0.09375
- w_down: bfloat16 [4096, 3584], P('ep'), may hold values from -0.1875 to 0.1875
- gate_resid: float32 [3584, 4096], P('edp', 'ep'), may hold values from -4 to 4
- up_resid: float32 [3584, 4096], P('edp', 'ep'), may hold values from -4 to 4
- down_resid: float32 [4096, 3584], P('ep', 'edp'), may hold values from -4 to 4
Outputs:
- kv_grad: bfloat16 [3584, 512], P(('edp', 'ep'))
- gate_grad: bfloat16 [3584, 4096], P('edp', 'ep')
- up_grad: bfloat16 [3584, 4096], P('edp', 'ep')
- down_grad: bfloat16 [4096, 3584], P('ep', 'edp')
The draws below stay inside these ranges and needn't reach their ends.
Inputs may be any that keep to these rules, and one draw needn't show every extreme that they name: `expert_ids`: each row names 2 different experts. Among the rows of one device no expert is named more than 80 times, and in some devices' rows one is named exactly 80 times.
All inputs are finite; a program needn't handle non-finite values.
Results may differ from the reference program's by a relative error of at most 0.019.
Values may be sent and summed in bfloat16 or wider, within the bound.
No kernel may reach another device: no remote copies, remote signals or barrier semaphores. Data moves between devices by JAX's collectives and lax.ppermute only.
A program may use at most 128 MiB of HBM per device.

```python
import math
import jax
import jax.numpy as jnp
import numpy as np
from jax import lax

D = 3584
FH = 1024
KVL = 512
TOP = 2
TOK_DEV = 128
EXPERTS = 4
CAP = 80
TOKENS = 4096
N_EDP = 2
N_EP = 16


def strengthened(array, stream_key, source, target, shards_of, factor):
    def block_of(dim):
        return (jnp.arange(array.shape[dim]) // (array.shape[dim] // shards_of)).reshape((-1,) + (1,) * (array.ndim - 1 - dim))

    one_side = jax.random.permutation(stream_key, shards_of)[block_of(target)]
    second = (block_of(target) + shards_of // 2) % shards_of
    return jnp.where((block_of(source) == one_side) | (block_of(source) == second), factor * array, array)


def shard_levels(stream_key, shape, pieces, low, high):
    gain, own = 1.0, jax.random.fold_in(stream_key, 6)
    for axis_at, blocks in pieces:
        steps = jnp.exp(jax.random.uniform(jax.random.fold_in(own, axis_at), (blocks,), jnp.float32, low / len(pieces), high / len(pieces)))
        gain = gain * jnp.repeat(steps, shape[axis_at] // blocks).reshape([-1 if axis == axis_at else 1 for axis in range(len(shape))])
    return gain


def routed_block(key, own, number, rows, number_of, top, limit, skew):
    sequence = jax.random.permutation(key, number_of)
    crowded, usual = load_shares(number_of, rows * top, limit, skew, True), load_shares(number_of, rows * top, limit, skew, False)
    places = jnp.arange(number_of)

    def named(lengths, offset_by):
        used = int((lengths > 0).sum())
        fixed = max(1, used // 4)
        shifted = fixed + (places - fixed + offset_by * (used - fixed)) % max(1, number_of - fixed)
        return jnp.zeros((number_of,), jnp.int32).at[sequence[jnp.where(places < fixed, places, shifted)]].set(jnp.asarray(lengths, jnp.int32))

    lengths = jnp.where(number % 4 == 0, named(crowded, number // 4), named(usual, number - number // 4 - 1))
    mixed = jax.random.permutation(jax.random.fold_in(own, 3), number_of)
    donor, receiver = mixed[0:number_of // 2 * 2:2], mixed[1:number_of // 2 * 2:2]
    margin = jnp.minimum(lengths[donor] - 1, limit - lengths[receiver]) // 2
    margin = jnp.where((donor == sequence[0]) | (receiver == sequence[0]) | (lengths[receiver] == 0), 0, jnp.maximum(margin, 0))
    shifted = jax.random.randint(jax.random.fold_in(own, 4), (number_of // 2,), 0, 1 << 20) % (margin + 1)
    lengths = lengths.at[donor].add(-shifted).at[receiver].add(shifted)
    items = jnp.searchsorted(jnp.cumsum(lengths), jnp.arange(rows * top), side="right").astype(jnp.int32)
    grid = items.reshape(top, rows).T
    grid = grid[jax.random.permutation(jax.random.fold_in(own, 1), rows)]
    offset_by = jax.random.randint(jax.random.fold_in(own, 2), (rows, 1), 0, top)
    return jnp.take_along_axis(grid, (jnp.arange(top)[None, :] + offset_by) % top, axis=1)


def load_shares(amount, total, reach, skew, full):
    weights = [(1 << 20) // math.isqrt(rank ** skew) + 1 for rank in range(1, amount + 1)]
    largest = reach if full else min(reach, max(-(-total // amount), total * weights[0] // sum(weights)))
    least = 1 if total - largest >= amount - 1 else 0
    counts, rest = [largest] + [least] * (amount - 1), total - largest - least * (amount - 1)
    while rest > 0:
        candidates = [i for i in range(1, amount) if counts[i] < largest] or [i for i in range(1, amount) if counts[i] < reach]
        pool, remaining = sum([weights[i] for i in candidates]), rest
        for i in candidates:
            extra = min(reach - counts[i], max(1, remaining * weights[i] // pool), rest)
            counts[i] = counts[i] + extra
            rest = rest - extra
    return np.array(counts)


def noise(stream_key, extent, scale, reach, shards=(), held_as=jnp.bfloat16):
    drawn = scale * jax.random.normal(stream_key, extent, jnp.float32)
    if shards:
        drawn = drawn * shard_levels(stream_key, extent, shards, -0.22, 0.18)
    return jnp.clip(drawn, -reach, reach).astype(held_as)


def heavy_noise(stream_key, dims, width, reach, pieces, heavy, held_as=jnp.bfloat16):
    entries = width * jax.random.normal(stream_key, dims, jnp.float32)
    if pieces:
        entries = entries * shard_levels(stream_key, dims, pieces, -0.22, 0.18)
    return jnp.clip(strengthened(entries, jax.random.fold_in(stream_key, 3), *heavy), -reach, reach).astype(held_as)


def setup_inputs(seed: int = 0) -> dict:
    seeds = jax.random.split(jax.random.key(seed), 15)
    attn_input = heavy_noise(seeds[0], (TOKENS, D), 1.0, 6.0, ((0, 32),), (0, 1, 32, 2.75))
    kv_gain = jnp.clip(1.0 + 0.15 * jax.random.normal(seeds[1], (D,), jnp.float32), 0.25, 1.75)
    latent_cot = noise(seeds[2], (TOKENS, KVL), TOKENS ** -0.5, 0.09375, ((0, 32),))
    attn_resid = noise(seeds[3], (D, KVL), 0.25, 4.0, ((0, 32),), jnp.float32)
    moe_input = heavy_noise(seeds[4], (TOKENS, D), 1.0, 6.0, ((0, 32),), (0, 1, 32, 2.75))
    moe_cot = noise(seeds[5], (TOKENS, D), (TOKENS * TOP // EXPERTS) ** -0.5, 0.125, ((0, 32),))
    expert_ids_keys = jax.random.split(jax.random.fold_in(seeds[6], 1), TOKENS // TOK_DEV)
    expert_ids_turns = jax.random.permutation(jax.random.fold_in(seeds[6], 3), TOKENS // TOK_DEV)
    expert_ids = jax.vmap(lambda own, number: routed_block(jax.random.fold_in(seeds[6], 2), own, number, TOK_DEV, EXPERTS, TOP, CAP, 1))(expert_ids_keys, expert_ids_turns).reshape((TOKENS, TOP))
    gate_probs = jnp.clip(0.2 + 0.8 * jax.random.uniform(seeds[7], (TOKENS, TOP), jnp.float32) ** shard_levels(seeds[7], (TOKENS, TOP), ((0, 32),), -0.2, 0.2), 0.2, 1.0)
    w_gate = noise(seeds[8], (D, EXPERTS * FH), D ** -0.5, 0.09375, ((1, 16),))
    w_up = noise(seeds[9], (D, EXPERTS * FH), D ** -0.5, 0.09375, ((1, 16),))
    w_down = noise(seeds[10], (EXPERTS * FH, D), FH ** -0.5, 0.1875, ((0, 16),))
    gate_resid = noise(seeds[11], (D, EXPERTS * FH), 0.25, 4.0, ((0, 2), (1, 16)), jnp.float32)
    up_resid = noise(seeds[12], (D, EXPERTS * FH), 0.25, 4.0, ((0, 2), (1, 16)), jnp.float32)
    down_resid = noise(seeds[13], (EXPERTS * FH, D), 0.25, 4.0, ((0, 16), (1, 2)), jnp.float32)
    return dict(attn_input=attn_input, kv_gain=kv_gain, latent_cot=latent_cot, attn_resid=attn_resid, moe_input=moe_input, moe_cot=moe_cot, expert_ids=expert_ids, gate_probs=gate_probs, w_gate=w_gate, w_up=w_up, w_down=w_down, gate_resid=gate_resid, up_resid=up_resid, down_resid=down_resid)


epsilon = 1e-06

def contract_rows(left, right):
    return lax.dot_general(left, right, (((0,), (0,)), ((), ())), preferred_element_type=jnp.float32)

def slot_tables(expert_ids, gate_probs):
    labels = jnp.arange(EXPERTS, dtype=jnp.int32)
    one_hot = (expert_ids[:, :, None] == labels[None, None, :]).astype(jnp.int32)
    chosen = lax.optimization_barrier(jnp.sum(one_hot, axis=1))
    weight = lax.optimization_barrier(jnp.sum(one_hot.astype(jnp.float32) * gate_probs[:, :, None], axis=1))
    position = jnp.cumsum(chosen, axis=0) - chosen
    slot_ids = jnp.arange(CAP, dtype=jnp.int32)
    dispatch = (chosen[None, :, :] > 0) & (position[None, :, :] == slot_ids[:, None, None])
    return (jnp.transpose(dispatch, (2, 0, 1)).astype(jnp.float32), weight)

def device_slots(inputs, cots, expert_ids, gate_probs):
    dispatch, weight = slot_tables(expert_ids, gate_probs)
    sent_in = jnp.einsum('ect,td->ecd', dispatch, inputs.astype(jnp.float32)).astype(jnp.bfloat16)
    sent_cot = jnp.einsum('ect,td->ecd', dispatch, cots.astype(jnp.float32))
    slot_weight = jnp.einsum('ect,te->ec', dispatch, weight)
    return (sent_in, (sent_cot * slot_weight[:, :, None]).astype(jnp.bfloat16))

def group_terms(inputs, cots, expert_ids, gate_probs, w_gate, w_up, w_down):
    sent_in, sent_cot = jax.vmap(device_slots)(inputs, cots, expert_ids, gate_probs)

    def per_expert(index):
        rows_in = lax.dynamic_index_in_dim(sent_in, index, 1, keepdims=False).reshape(N_EP * CAP, D)
        rows_cot = lax.dynamic_index_in_dim(sent_cot, index, 1, keepdims=False).reshape(N_EP * CAP, D)
        gate_cols = lax.dynamic_slice_in_dim(w_gate, index * FH, FH, 1)
        up_cols = lax.dynamic_slice_in_dim(w_up, index * FH, FH, 1)
        down_rows = lax.dynamic_slice_in_dim(w_down, index * FH, FH, 0)
        gate_proj = jnp.dot(rows_in, gate_cols, preferred_element_type=jnp.float32)
        up_proj = jnp.dot(rows_in, up_cols, preferred_element_type=jnp.float32)
        sigmoid_gate = jax.nn.sigmoid(gate_proj)
        active = (gate_proj * sigmoid_gate * up_proj).astype(jnp.bfloat16)
        back_grad = lax.dot_general(rows_cot, down_rows, (((1,), (1,)), ((), ())), preferred_element_type=jnp.float32)
        up_rows = (back_grad * gate_proj * sigmoid_gate).astype(jnp.bfloat16)
        gate_rows = (back_grad * up_proj * sigmoid_gate * (1.0 + gate_proj * (1.0 - sigmoid_gate))).astype(jnp.bfloat16)
        return (contract_rows(rows_in, gate_rows).astype(jnp.bfloat16), contract_rows(rows_in, up_rows).astype(jnp.bfloat16), contract_rows(active, rows_cot).astype(jnp.bfloat16))
    return lax.map(per_expert, jnp.arange(EXPERTS, dtype=jnp.int32))

def reference(attn_input, kv_gain, latent_cot, attn_resid, moe_input, moe_cot, expert_ids, gate_probs, w_gate, w_up, w_down, gate_resid, up_resid, down_resid):
    values = attn_input.astype(jnp.float32)
    inv_rms = lax.rsqrt(lax.optimization_barrier(jnp.mean(values * values, axis=1, keepdims=True)) + epsilon)
    normed = (values * inv_rms * kv_gain[None, :]).astype(jnp.bfloat16)
    kv_grad = (contract_rows(normed, latent_cot) + attn_resid).astype(jnp.bfloat16)
    groups = (moe_input.reshape(N_EDP, N_EP, TOK_DEV, D), moe_cot.reshape(N_EDP, N_EP, TOK_DEV, D), expert_ids.reshape(N_EDP, N_EP, TOK_DEV, TOP), gate_probs.reshape(N_EDP, N_EP, TOK_DEV, TOP))

    def accumulate(carry, group):
        terms = group_terms(group[0], group[1], group[2], group[3], w_gate, w_up, w_down)
        return ((carry[0] + terms[0].astype(jnp.float32), carry[1] + terms[1].astype(jnp.float32), carry[2] + terms[2].astype(jnp.float32)), None)
    start = (jnp.zeros((EXPERTS, D, FH), jnp.float32), jnp.zeros((EXPERTS, D, FH), jnp.float32), jnp.zeros((EXPERTS, FH, D), jnp.float32))
    sums, _ = lax.scan(accumulate, start, groups)
    gate_sum = jnp.transpose(sums[0], (1, 0, 2)).reshape(D, EXPERTS * FH)
    up_sum = jnp.transpose(sums[1], (1, 0, 2)).reshape(D, EXPERTS * FH)
    down_sum = sums[2].reshape(EXPERTS * FH, D)
    gate_grad = (gate_sum + gate_resid).astype(jnp.bfloat16)
    up_grad = (up_sum + up_resid).astype(jnp.bfloat16)
    down_grad = (down_sum + down_resid).astype(jnp.bfloat16)
    return (kv_grad, gate_grad, up_grad, down_grad)
```

```python
import jax
import jax.numpy as jnp
from jax import lax
from jax.sharding import PartitionSpec as P

TOP = 2
SPLIT = 4

epsilon = 1e-06


def contract_rows(left, right):
    return lax.dot_general(
        left, right, (((0,), (0,)), ((), ())), preferred_element_type=jnp.float32
    )


def tie(value, *after):
    return lax.optimization_barrier((value,) + after)[0]


def swap_expert(value, k):
    n = lax.axis_size("ep")
    return lax.ppermute(value, "ep", [(i, i ^ (k * SPLIT)) for i in range(n)])


def swap_inner(value, k):
    n = lax.axis_size("ep")
    return lax.ppermute(value, "ep", [(i, i ^ k) for i in range(n)])


def swap_copy(value, k):
    n = lax.axis_size("edp")
    return lax.ppermute(value, "edp", [(i, i ^ k) for i in range(n)])


def pick(stacked, index):
    return lax.dynamic_index_in_dim(stacked, index, 0, keepdims=False)


def latent_partial(attn_input, kv_gain, latent_cot):
    values = attn_input.astype(jnp.float32)
    inv_rms = lax.rsqrt(jnp.mean(values * values, axis=1, keepdims=True) + epsilon)
    normed = (values * inv_rms * kv_gain[None, :]).astype(jnp.bfloat16)
    return contract_rows(normed, latent_cot)


def scatter_sum(stacked, mine, swap, count):
    total = pick(stacked, mine)
    for k in range(1, count):
        total = total + swap(pick(stacked, mine ^ k).astype(jnp.bfloat16), k).astype(jnp.float32)
    return total


def slot_tables(expert_ids, gate_probs, labels, capacity):
    one_hot = (expert_ids[:, :, None] == labels[None, None, :]).astype(jnp.int32)
    chosen = jnp.sum(one_hot, axis=1)
    weight = jnp.sum(one_hot.astype(jnp.float32) * gate_probs[:, :, None], axis=1)
    position = jnp.cumsum(chosen, axis=0) - chosen
    slot_ids = jnp.arange(capacity, dtype=jnp.int32)
    dispatch = (chosen[None, :, :] > 0) & (position[None, :, :] == slot_ids[:, None, None])
    return (jnp.transpose(dispatch, (2, 0, 1)), weight)


def spread(block, k):
    got = block if k == 0 else swap_expert(block, k)
    across = swap_inner(got, 2)
    pair = jnp.concatenate([got, across], axis=0)
    other = swap_inner(pair, 1)
    return jnp.concatenate([pair, other], axis=0)


def body(
    attn_input,
    kv_gain,
    latent_cot,
    attn_resid,
    moe_input,
    moe_cot,
    expert_ids,
    gate_probs,
    w_gate,
    w_up,
    w_down,
    gate_resid,
    up_resid,
    down_resid,
):
    experts = lax.axis_size("ep") // SPLIT
    copies = lax.axis_size("edp")
    capacity = 5 * moe_input.shape[0] * TOP // (4 * experts)
    here = lax.axis_index("ep")
    my_expert, my_place = here // SPLIT, here % SPLIT
    my_copy = lax.axis_index("edp")

    labels = my_expert ^ jnp.arange(experts, dtype=jnp.int32)
    dispatch, weight = slot_tables(expert_ids, gate_probs, labels, capacity)
    dispatch_half = dispatch.astype(jnp.bfloat16)
    sent_in = jnp.einsum(
        "ect,td->ecd", dispatch_half, moe_input, preferred_element_type=jnp.float32
    ).astype(jnp.bfloat16)
    sent_cot = jnp.einsum("ect,td->ecd", dispatch_half, moe_cot, preferred_element_type=jnp.float32)
    slot_weight = jnp.einsum("ect,te->ec", dispatch.astype(jnp.float32), weight)
    sent_cot = (sent_cot * slot_weight[:, :, None]).astype(jnp.bfloat16)

    kv_part = latent_partial(attn_input, kv_gain, latent_cot)
    latent_rows = kv_part.shape[0] // (copies * experts * SPLIT)

    rows_in = [spread(sent_in[k], k) for k in range(experts)]
    rows_cot = [spread(sent_cot[k], k) for k in range(experts)]

    kv = kv_part.reshape((copies, -1) + kv_part.shape[1:])
    kv = scatter_sum(kv, my_copy, swap_copy, copies)
    kv = tie(kv, rows_cot[-1])
    kv = kv.reshape((experts, SPLIT, latent_rows) + kv.shape[1:]).transpose(1, 0, 2, 3)
    kv = scatter_sum(kv, my_place, swap_inner, SPLIT)
    kv = scatter_sum(kv, my_expert, swap_expert, experts)
    kv_grad = (kv + attn_resid).astype(jnp.bfloat16)

    gate_sum = up_sum = down_sum = 0.0
    for k in range(experts):
        gate_proj = jnp.dot(rows_in[k], w_gate, preferred_element_type=jnp.float32)
        up_proj = jnp.dot(rows_in[k], w_up, preferred_element_type=jnp.float32)
        sigmoid_gate = jax.nn.sigmoid(gate_proj)
        active = (gate_proj * sigmoid_gate * up_proj).astype(jnp.bfloat16)
        back_grad = lax.dot_general(
            rows_cot[k], w_down, (((1,), (1,)), ((), ())), preferred_element_type=jnp.float32
        )
        up_rows = (back_grad * gate_proj * sigmoid_gate).astype(jnp.bfloat16)
        gate_rows = (
            back_grad * up_proj * sigmoid_gate * (1.0 + gate_proj * (1.0 - sigmoid_gate))
        ).astype(jnp.bfloat16)
        down_sum = contract_rows(active, rows_cot[k]) + down_sum
        gate_sum = contract_rows(rows_in[k], gate_rows) + gate_sum
        up_sum = contract_rows(rows_in[k], up_rows) + up_sum

    def over_copies(total, resid, dim):
        if dim == 1:
            stacked = total.reshape(total.shape[0], copies, -1).transpose(1, 0, 2)
        else:
            stacked = total.reshape((copies, -1) + total.shape[1:])
        return (scatter_sum(stacked, my_copy, swap_copy, copies) + resid).astype(jnp.bfloat16)

    down_grad = over_copies(down_sum, down_resid, 1)
    gate_grad = over_copies(gate_sum, gate_resid, 0)
    up_grad = over_copies(up_sum, up_resid, 0)
    return (kv_grad, gate_grad, up_grad, down_grad)


def solution(mesh):
    placed = (
        P(("edp", "ep"), None),
        P(),
        P(("edp", "ep"), None),
        P(("edp", "ep"), None),
        P(("edp", "ep"), None),
        P(("edp", "ep"), None),
        P(("edp", "ep"), None),
        P(("edp", "ep"), None),
        P(None, "ep"),
        P(None, "ep"),
        P("ep", None),
        P("edp", "ep"),
        P("edp", "ep"),
        P("ep", "edp"),
    )
    return jax.shard_map(
        body,
        mesh=mesh,
        in_specs=placed,
        out_specs=(P(("edp", "ep"), None), P("edp", "ep"), P("edp", "ep"), P("ep", "edp")),
        check_vma=False,
    )
```
